256 devices in a mesh: row: 8 (over y, core), col: 4 (over x), layer: 8 (over z).
Axes of the slice: x: 4, y: 4, z: 8, core: 2. Of those that a mesh axis runs over, the one named last changes fastest.
Arguments:
- hamiltonian: bfloat16 [5120, 5120], P(('row', 'layer'), 'col'), may hold values from -1.2 to 1.2, as said below
- tile_pattern: int32 [40, 40], replicated, may hold values from 0 to 1, as said below
- n_occ: int32 [1], replicated, may hold values from 1024 to 4095
- mu: float32 [1], replicated, may hold values from -0.2 to 0.2
- gamma: float32 [1], replicated, may hold values from 0.25 to 0.4
Outputs:
- density: float32 [5120, 5120], P(('row', 'layer'), 'col')
The draws below stay inside these ranges and needn't reach their ends.
Inputs may be any that keep to these rules, and one draw needn't show every extreme that they name: `tile_pattern`: Symmetric, 0 or 1, with ones on the diagonal and next to it. `hamiltonian`: Symmetric; its eigenvalues lie within -1.8 and 1.8.
All inputs are finite; a program needn't handle non-finite values.
Results may differ from the reference program's by a relative error of at most 0.0055.
Values may be sent and summed in bfloat16 or wider, within the bound.
A program may use at most 64 MiB of HBM per device.

```python
import jax
import jax.numpy as jnp

TILE = 128
STEPS = 2
TILES = 40
NORB = 5120


def tile_layout(key):
    row_ids = jnp.arange(TILES, dtype=jnp.int32)[:, None]
    col_ids = jnp.arange(TILES, dtype=jnp.int32)[None, :]
    tile_score = jax.random.randint(key, (TILES, TILES), 0, 100, dtype=jnp.int32)
    tile_score = jnp.where(row_ids <= col_ids, tile_score, tile_score.T)
    chance = 3 + 30 * (row_ids + col_ids) // (2 * TILES)
    near_diag = jnp.abs(row_ids - col_ids) <= 1
    return jnp.where(near_diag | (tile_score < chance), 1, 0).astype(jnp.int32)


def draw_tile_pattern(key, part):
    return tile_layout(jax.random.fold_in(key, 7))


def draw_hamiltonian(key, part):
    pattern = tile_layout(jax.random.fold_in(key, 7))
    dense_mask = jnp.repeat(jnp.repeat(pattern, TILE, 0), TILE, 1).astype(jnp.float32)
    row_count = jnp.sum(dense_mask, axis=1)
    row_weight = row_count ** (-0.25)
    first_key, second_key = jax.random.split(jax.random.fold_in(key, 13))
    noise_field = jax.random.normal(first_key, (NORB, NORB), jnp.float32)
    onsite = jax.random.uniform(second_key, (NORB,), jnp.float32, -0.2, 0.2)
    noise_field = jnp.clip((noise_field + noise_field.T) * 0.7071, -4.0, 4.0)
    identity = jnp.eye(NORB, dtype=jnp.float32)
    scaling = 0.65 * row_weight[:, None] * row_weight[None, :]
    coupled = dense_mask * scaling * noise_field * (1.0 - identity)
    return (coupled + identity * onsite[None, :]).astype(jnp.bfloat16)


def setup_inputs(seed: int = 0) -> dict:
    streams_of = jax.random.split(jax.random.key(seed), 6)
    hamiltonian = draw_hamiltonian(jax.random.fold_in(streams_of[5], 71), 0)
    tile_pattern = draw_tile_pattern(jax.random.fold_in(streams_of[5], 71), 0)
    n_occ = jax.random.randint(streams_of[2], (1,), NORB // 5, 4 * NORB // 5).astype(jnp.int32)
    mu = jnp.clip(jax.random.uniform(streams_of[3], (1,), jnp.float32, -0.2, 0.2), -0.2, 0.2)
    gamma = jnp.clip(jax.random.uniform(streams_of[4], (1,), jnp.float32, 0.25, 0.4), 0.25, 0.4)
    return dict(hamiltonian=hamiltonian, tile_pattern=tile_pattern, n_occ=n_occ, mu=mu, gamma=gamma)


def reference(hamiltonian, tile_pattern, n_occ, mu, gamma):
    mask = jnp.repeat(jnp.repeat(tile_pattern, TILE, 0), TILE, 1).astype(jnp.float32)
    identity = jnp.eye(NORB, dtype=jnp.float32)
    filling = n_occ[0].astype(jnp.float32) / NORB
    start = mask * (filling * identity + gamma[0] * (mu[0] * identity - hamiltonian.astype(jnp.float32)))
    current = start.astype(jnp.bfloat16)
    result = start
    for iteration in range(STEPS):
        square = mask * jnp.dot(current, current, preferred_element_type=jnp.float32)
        cube = mask * jnp.dot(square.astype(jnp.bfloat16), current, preferred_element_type=jnp.float32)
        result = 3.0 * square - 2.0 * cube
        current = result.astype(jnp.bfloat16)
    return result
```

```python
import functools
import heapq

import jax
import jax.numpy as jnp
from jax import lax
from jax.experimental import pallas as pl
from jax.experimental.pallas import tpu as pltpu
from jax.sharding import PartitionSpec as P

TILE = 128
LANES = 128
STEPS = 2
MESH = pl.DeviceIdType.MESH
CHUNK = 256


def gather_schedule(ny, nz, rows, cols, first_cols, rate=46.65, lat=1.9):
    ring = {"y": ny, "z": nz}
    free, events, ops, count = {}, [], [], 0

    def send(t, axis, sign, piece, hops):
        nonlocal count
        h, dy, dz, c0, w = piece
        begin = max(t, free.get((axis, sign), 0.0))
        end = begin + rows * w * 2 / rate / 1000
        free[axis, sign] = end
        landed = (h, dy - sign, dz, c0, w) if axis == "y" else (h, dy, dz - sign, c0, w)
        heapq.heappush(events, (end + lat, count, axis, sign, landed, hops + 1))
        ops.append(("send", axis, sign, piece, count))
        count += 1

    def forward(t, axis, sign, piece, hops):
        h, dy, dz, c0, w = piece
        half = ring[axis] // 2
        if hops < half - 1:
            send(t, axis, sign, piece, hops)
        elif hops == half - 1:
            part = (w // 2 + (0 if c0 <= first_cols else LANES - 1)) // LANES * LANES
            send(t, axis, sign, (h, dy, dz, c0, part) if sign > 0 else (h, dy, dz, c0 + part, w - part), hops)

    own = {1: (1, 0, 0, 0, first_cols), 2: (2, 0, 0, first_cols, cols - first_cols)}
    for turn in (0, 1):
        for sign in (1, -1):
            send(0.0, "y", sign, own[1 + turn], 0)
            send(0.0, "z", sign, own[2 - turn], 0)
    while events:
        t, receive, axis, sign, piece, hops = heapq.heappop(events)
        ops.append(("wait", piece, receive))
        forward(t, axis, sign, piece, hops)
        if axis == ("y" if piece[0] == 1 else "z"):
            for way in (1, -1):
                send(t, "z" if axis == "y" else "y", way, piece, 0)
    return ops, count


def kernel(sizes, ops, h_ref, pattern_ref, occ_ref, mu_ref, gamma_ref, out_ref,
           band, left, mask, square, total, current, band_recv, band_send, pair_sem, left_recv, left_send):
    nx, ny, nz, rows, cols = sizes
    order = nx * cols
    half = ny * nz * rows
    row, x, z = lax.axis_index("row"), lax.axis_index("col"), lax.axis_index("layer")
    y, core = row // 2, row % 2
    partner = {"row": 2 * y + 1 - core}

    def there(axis, sign):
        if axis == "y":
            return {"row": 2 * ((y + sign + ny) % ny) + core}
        if axis == "z":
            return {"layer": (z + sign + nz) % nz}
        return {"col": (x + sign + nx) % nx}

    row0 = pl.multiple_of((row * nz + z) * rows, 16)
    col0 = pl.multiple_of(x * cols, 128)

    barrier = pltpu.get_barrier_semaphore()
    friends = [partner] + [there(a, g) for a in ("x", "y", "z") for g in (1, -1)]
    for friend in friends:
        pl.semaphore_signal(barrier, inc=1, device_id=friend, device_id_type=MESH)

    tiles = pattern_ref.shape[0]
    row_tile = (row0 + lax.broadcasted_iota(jnp.int32, (rows, tiles), 0)) // TILE
    row_hot = (row_tile == lax.broadcasted_iota(jnp.int32, (rows, tiles), 1)).astype(jnp.bfloat16)
    col_tile = (col0 + lax.broadcasted_iota(jnp.int32, (tiles, cols), 1)) // TILE
    col_hot = (col_tile == lax.broadcasted_iota(jnp.int32, (tiles, cols), 0)).astype(jnp.bfloat16)
    picked = jnp.dot(row_hot, pattern_ref[...].astype(jnp.float32).astype(jnp.bfloat16),
                     preferred_element_type=jnp.float32)
    mask[...] = jnp.dot(picked.astype(jnp.bfloat16), col_hot, preferred_element_type=jnp.float32)
    identity = (row0 + lax.broadcasted_iota(jnp.int32, (rows, cols), 0)
                == col0 + lax.broadcasted_iota(jnp.int32, (rows, cols), 1)).astype(jnp.float32)
    filling = occ_ref[0].astype(jnp.float32) / order
    start = mask[...] * (filling * identity + gamma_ref[0] * (mu_ref[0] * identity - h_ref[...].astype(jnp.float32)))
    current[...] = start.astype(jnp.bfloat16)

    pl.semaphore_wait(barrier, len(friends))

    def step(s, carry):
        def block(piece):
            _, dy, dz, c0, w = piece
            origin = (2 * ((y + dy + ny) % ny) + core) * nz + (z + dz + nz) % nz
            return band.at[s, pl.ds(pl.multiple_of(origin * rows, 16), rows), pl.ds(c0, w)]

        def to_partner(ref):
            return pltpu.make_async_remote_copy(
                src_ref=ref, dst_ref=ref, send_sem=pair_sem.at[s, 0], recv_sem=pair_sem.at[s, 1],
                device_id=partner, device_id_type=MESH)

        def along(axis, sign, piece, receive):
            ref = block(piece)
            return pltpu.make_async_remote_copy(
                src_ref=ref, dst_ref=ref, send_sem=band_send.at[s], recv_sem=band_recv.at[s, receive],
                device_id=there(axis, sign), device_id_type=MESH)

        def left_block(which, dx, c0, w):
            at = pl.multiple_of(((x + dx + nx) % nx) * cols + c0, 128)
            return left.at[s, which, :, pl.ds(at, w)]

        def left_copy(which, sign, dx, c0, w, receive):
            ref = left_block(which, dx, c0, w)
            return pltpu.make_async_remote_copy(
                src_ref=ref, dst_ref=ref, send_sem=left_send.at[s, which], recv_sem=left_recv.at[s, which, receive],
                device_id=there("x", sign), device_id_type=MESH)

        band[s, pl.ds(row0, rows), :] = current[...]
        left[s, 0, :, pl.ds(col0, cols)] = current[...]

        mid = cols // 2
        left_copy(0, 1, 0, 0, cols, 0).start()
        left_copy(0, -1, 0, 0, cols, 1).start()

        told, forwarded = False, False
        for op in ops:
            if op[0] == "send":
                along(*op[1:]).start()
                continue
            if not told:
                told = True
                to_partner(band.at[s, pl.ds(row0, rows), :]).start()
            _, piece, receive = op
            along("y", 1, piece, receive).wait_recv()
            to_partner(block(piece)).start()
            if not forwarded and receive > 12:
                forwarded = True
                left_copy(0, 1, -1, 0, cols, 0).wait_recv()
                left_copy(0, 1, -1, 0, mid, 2).start()
                left_copy(0, -1, 1, 0, cols, 1).wait_recv()
                left_copy(0, -1, 1, mid, mid, 3).start()
        left_copy(0, 1, -2, 0, mid, 2).wait_recv()
        left_copy(0, -1, -2, mid, mid, 3).wait_recv()
        everything = band.at[s, pl.ds(0, half), :]
        pltpu.make_async_copy(everything, everything, pair_sem.at[s, 1]).wait()

        def chunk_parts(c0):
            ways = []
            if c0 < mid:
                ways.append((1, c0, min(CHUNK, mid - c0)))
            if c0 + CHUNK > mid:
                begin = max(c0, mid)
                ways.append((-1, begin, c0 + CHUNK - begin))
            return ways

        n_chunks = cols // CHUNK
        walk = sorted(range(n_chunks), key=lambda n: min(n, n_chunks - 1 - n))
        for n in walk:
            c0 = n * CHUNK
            product = jnp.dot(left[s, 0], band[s, :, c0:c0 + CHUNK], preferred_element_type=jnp.float32)
            product = mask[:, c0:c0 + CHUNK] * product
            square[:, c0:c0 + CHUNK] = product
            left[s, 1, :, pl.ds(pl.multiple_of(col0 + c0, 128), CHUNK)] = product.astype(jnp.bfloat16)
            for way, sign in enumerate((1, -1)):
                left_copy(1, sign, 0, c0, CHUNK, 2 * n + way).start()
        far = {}
        for n in walk:
            c0 = n * CHUNK
            for way, sign in enumerate((1, -1)):
                left_copy(1, sign, -sign, c0, CHUNK, 2 * n + way).wait_recv()
                for go, begin, width in chunk_parts(c0):
                    if go == sign:
                        far[begin] = (sign, begin, width, 2 * n_chunks + len(far))
                        left_copy(1, sign, -sign, begin, width, far[begin][3]).start()

        def add(dx, first):
            at = pl.multiple_of(((x + dx + nx) % nx) * cols, 128)
            for n in range(n_chunks):
                c0 = n * CHUNK
                part = jnp.dot(left[s, 1, :, pl.ds(at, cols)], band[s, pl.ds(at, cols), c0:c0 + CHUNK],
                               preferred_element_type=jnp.float32)
                if first:
                    total[:, c0:c0 + CHUNK] = part
                else:
                    total[:, c0:c0 + CHUNK] += part

        add(0, True)
        add(-1, False)
        add(1, False)
        for sign, begin, width, receive in far.values():
            left_copy(1, sign, -2, begin, width, receive).wait_recv()
        add(2, False)
        result = 3.0 * square[...] - 2.0 * (mask[...] * total[...])
        out_ref[...] = result
        current[...] = result.astype(jnp.bfloat16)

        sent = band.at[s, pl.ds(0, half - rows), :]
        pltpu.make_async_copy(sent, sent, band_send.at[s]).wait()
        pltpu.make_async_copy(everything, everything, pair_sem.at[s, 0]).wait()
        for which in (0, 1):
            ref = left.at[s, which, :, pl.ds(0, 3 * cols)]
            pltpu.make_async_copy(ref, ref, left_send.at[s, which]).wait()
        return carry

    lax.fori_loop(0, STEPS, step, 0)


def solution(mesh):
    nx, ny, nz = mesh.shape["col"], mesh.shape["row"] // 2, mesh.shape["layer"]

    def shards(hamiltonian, tile_pattern, n_occ, mu, gamma):
        rows, cols = hamiltonian.shape
        order = nx * cols
        ops, count = gather_schedule(ny, nz, rows, cols, 512)
        vmem = pl.BlockSpec(memory_space=pltpu.VMEM)
        smem = pl.BlockSpec(memory_space=pltpu.SMEM)
        return pl.pallas_call(
            functools.partial(kernel, (nx, ny, nz, rows, cols), ops),
            out_shape=jax.ShapeDtypeStruct((rows, cols), jnp.float32),
            in_specs=[vmem, vmem, smem, smem, smem],
            out_specs=vmem,
            scratch_shapes=[
                pltpu.VMEM((STEPS, order, cols), jnp.bfloat16),
                pltpu.VMEM((STEPS, 2, rows, order), jnp.bfloat16),
                pltpu.VMEM((rows, cols), jnp.float32),
                pltpu.VMEM((rows, cols), jnp.float32),
                pltpu.VMEM((rows, cols), jnp.float32),
                pltpu.VMEM((rows, cols), jnp.bfloat16),
                pltpu.SemaphoreType.DMA((STEPS, count)),
                pltpu.SemaphoreType.DMA((STEPS,)),
                pltpu.SemaphoreType.DMA((STEPS, 2)),
                pltpu.SemaphoreType.DMA((STEPS, 2, 16)),
                pltpu.SemaphoreType.DMA((STEPS, 2)),
            ],
            compiler_params=pltpu.CompilerParams(
                collective_id=0, has_side_effects=True, vmem_limit_bytes=48 * 2**20),
            name="purify",
        )(hamiltonian, tile_pattern, n_occ, mu, gamma)

    placed = (P(("row", "layer"), "col"), P(), P(), P(), P())
    return jax.shard_map(
        shards, mesh=mesh, in_specs=placed, out_specs=P(("row", "layer"), "col"), check_vma=False
    )
```

```python
import functools
import heapq

import jax
import jax.numpy as jnp
from jax import lax
from jax.experimental import pallas as pl
from jax.experimental.pallas import tpu as pltpu
from jax.sharding import PartitionSpec as P

TILE = 128
LANES = 128
STEPS = 2
MESH = pl.DeviceIdType.MESH
CHUNK = 256
CHUNKS = ((0, "y"), (1, "z"), (3, "y"), (2, "z"), (4, "z"))


def gather_schedule(ny, nz, rows, chunks, rate=46.65, lat=1.9, ahead=0.8, partner=1.5, late=3.1, product=0.7, hop=3.0):
    ring = {"y": ny, "z": nz}
    free, events, ops, waiting = {}, [], [], {}
    missing = {(n, dy): (nz - (dy == 0)) * c[1] for n, c in enumerate(chunks) for dy in range(ny)}
    blocks = [0] * len(chunks)
    count = 0

    def later(t, *event):
        heapq.heappush(events, (t, len(ops), len(events), *event))

    def offer(axis, sign, piece, hops):
        n, dy, dz, c0, w = piece
        half = ring[axis] // 2
        if hops == half:
            return
        if hops == half - 1:
            if w > LANES:
                cut = w // 2 // LANES * LANES
                piece = (n, dy, dz, c0, cut) if sign > 0 else (n, dy, dz, c0 + cut, w - cut)
            elif (sign > 0) != (c0 // LANES % 2 == 0):
                return
        second = axis != chunks[n][2]
        waiting.setdefault((axis, sign), []).append(((n + late * second, second, hops), piece, hops))

    def pump(t):
        nonlocal count
        for (axis, sign), queue in waiting.items():
            while queue and free.get((axis, sign), 0.0) - ahead <= t:
                queue.sort(key=lambda entry: entry[0])
                _, piece, hops = queue.pop(0)
                n, dy, dz, c0, w = piece
                end = max(t, free.get((axis, sign), 0.0)) + rows * w * 2 / rate / 1000
                free[axis, sign] = end
                ops.append(("send", axis, sign, piece, count))
                landed = (n, dy - sign, dz, c0, w) if axis == "y" else (n, dy, dz - sign, c0, w)
                later(end + lat, "land", axis, sign, landed, hops + 1, count)
                later(end - ahead, "free")
                count += 1

    for n, (c0, w, _) in enumerate(chunks):
        for axis in "yz":
            for sign in (1, -1):
                offer(axis, sign, (n, 0, 0, c0, w), 0)
    pump(0.0)
    while events:
        t, _, _, kind, *rest = heapq.heappop(events)
        if kind == "land":
            axis, sign, piece, hops, receive = rest
            n, dy, dz, c0, w = piece
            ops.append(("wait", piece, receive))
            offer(axis, sign, piece, hops)
            if axis == chunks[n][2]:
                for way in (1, -1):
                    offer("z" if axis == "y" else "y", way, piece, 0)
            missing[n, dy % ny] -= w
            if missing[n, dy % ny] == 0:
                ops.append(("pair", n, dy % ny))
                blocks[n] += 1
                if blocks[n] == ny:
                    later(t + partner, "square", n)
        elif kind == "square":
            ops.append(("square", rest[0]))
            later(t + product + hop, "relay", rest[0])
        elif kind == "relay":
            ops.append(("relay", rest[0]))
        pump(t)
    return ops, count


def kernel(sizes, chunks, ops, h_ref, pattern_ref, occ_ref, mu_ref, gamma_ref, out_ref,
           band, left, mask, square, total, current, band_recv, band_send, pair_recv, pair_send, left_recv, left_send):
    nx, ny, nz, rows, cols = sizes
    order = nx * cols
    half = ny * nz * rows
    row, x, z = lax.axis_index("row"), lax.axis_index("col"), lax.axis_index("layer")
    y, core = row // 2, row % 2
    partner = {"row": 2 * y + 1 - core}
    to = {}
    for sign in (1, -1):
        to["x", sign] = {"col": (x + sign + nx) % nx}
        to["y", sign] = {"row": 2 * ((y + sign + ny) % ny) + core}
        to["z", sign] = {"layer": (z + sign + nz) % nz}
    row0 = pl.multiple_of((row * nz + z) * rows, 16)
    col0 = pl.multiple_of(x * cols, 128)

    barrier = pltpu.get_barrier_semaphore()
    friends = [partner, *to.values()]
    for friend in friends:
        pl.semaphore_signal(barrier, inc=1, device_id=friend, device_id_type=MESH)

    tiles = pattern_ref.shape[0]
    row_tile = (row0 + lax.broadcasted_iota(jnp.int32, (rows, tiles), 0)) // TILE
    row_hot = (row_tile == lax.broadcasted_iota(jnp.int32, (rows, tiles), 1)).astype(jnp.bfloat16)
    col_tile = (col0 + lax.broadcasted_iota(jnp.int32, (tiles, cols), 1)) // TILE
    col_hot = (col_tile == lax.broadcasted_iota(jnp.int32, (tiles, cols), 0)).astype(jnp.bfloat16)
    picked = jnp.dot(row_hot, pattern_ref[...].astype(jnp.float32).astype(jnp.bfloat16),
                     preferred_element_type=jnp.float32)
    mask[...] = jnp.dot(picked.astype(jnp.bfloat16), col_hot, preferred_element_type=jnp.float32)
    identity = (row0 + lax.broadcasted_iota(jnp.int32, (rows, cols), 0)
                == col0 + lax.broadcasted_iota(jnp.int32, (rows, cols), 1)).astype(jnp.float32)
    filling = occ_ref[0].astype(jnp.float32) / order
    start = mask[...] * (filling * identity + gamma_ref[0] * (mu_ref[0] * identity - h_ref[...].astype(jnp.float32)))
    current[...] = start.astype(jnp.bfloat16)

    pl.semaphore_wait(barrier, len(friends))

    def step(s, carry):
        def along(axis, sign, piece, receive):
            _, dy, dz, c0, w = piece
            origin = (2 * ((y + dy + ny) % ny) + core) * nz + (z + dz + nz) % nz
            ref = band.at[s, pl.ds(pl.multiple_of(origin * rows, 16), rows), pl.ds(c0, w)]
            return pltpu.make_async_remote_copy(
                src_ref=ref, dst_ref=ref, send_sem=band_send.at[s], recv_sem=band_recv.at[s, receive],
                device_id=to[axis, sign], device_id_type=MESH)

        def to_partner(n, dy):
            begin = pl.multiple_of((2 * ((y + dy) % ny) + core) * nz * rows, 16)
            ref = band.at[s, pl.ds(begin, nz * rows), pl.ds(*chunks[n][:2])]
            return pltpu.make_async_remote_copy(
                src_ref=ref, dst_ref=ref, send_sem=pair_send.at[s], recv_sem=pair_recv.at[s, n],
                device_id=partner, device_id_type=MESH)

        def along_x(which, sign, dx, c0, w, receive):
            at = pl.multiple_of(((x + dx + nx) % nx) * cols + c0, 128)
            ref = left.at[s, which, :, pl.ds(at, w)]
            return pltpu.make_async_remote_copy(
                src_ref=ref, dst_ref=ref, send_sem=left_send.at[s, which], recv_sem=left_recv.at[s, which, receive],
                device_id=to["x", sign], device_id_type=MESH)

        band[s, pl.ds(row0, rows), :] = current[...]
        left[s, 0, :, pl.ds(col0, cols)] = current[...]

        mid = cols // 2

        def left_begin():
            along_x(0, 1, 0, 0, cols, 0).start()
            along_x(0, -1, 0, 0, cols, 1).start()

        def left_relay():
            along_x(0, 1, -1, 0, cols, 0).wait_recv()
            along_x(0, 1, -1, 0, mid, 2).start()
            along_x(0, -1, 1, 0, cols, 1).wait_recv()
            along_x(0, -1, 1, mid, mid, 3).start()

        def left_end():
            along_x(0, 1, -2, 0, mid, 2).wait_recv()
            along_x(0, -1, -2, mid, mid, 3).wait_recv()

        def square_chunk(n):
            c0, w, _ = chunks[n]
            arrived = band.at[s, pl.ds(0, half), pl.ds(c0, w)]
            pltpu.make_async_copy(arrived, arrived, pair_recv.at[s, n]).wait()
            product = jnp.dot(left[s, 0], band[s, :, c0:c0 + w], preferred_element_type=jnp.float32)
            product = mask[:, c0:c0 + w] * product
            square[:, c0:c0 + w] = product
            left[s, 1, :, pl.ds(pl.multiple_of(col0 + c0, 128), w)] = product.astype(jnp.bfloat16)
            along_x(1, 1, 0, c0, w, 4 * n).start()
            along_x(1, -1, 0, c0, w, 4 * n + 1).start()

        def relay_chunk(n):
            c0, w, _ = chunks[n]
            cut = w // 2
            along_x(1, 1, -1, c0, w, 4 * n).wait_recv()
            along_x(1, 1, -1, c0, cut, 4 * n + 2).start()
            along_x(1, -1, 1, c0, w, 4 * n + 1).wait_recv()
            along_x(1, -1, 1, c0 + cut, w - cut, 4 * n + 3).start()

        def far_chunk(n):
            c0, w, _ = chunks[n]
            cut = w // 2
            along_x(1, 1, -2, c0, cut, 4 * n + 2).wait_recv()
            along_x(1, -1, -2, c0 + cut, w - cut, 4 * n + 3).wait_recv()

        def cube_part(dx, k0, width, first=False):
            at = pl.multiple_of(((x + dx + nx) % nx) * cols + k0, 128)
            for c0, w, _ in chunks:
                part = jnp.dot(left[s, 1, :, pl.ds(at, width)], band[s, pl.ds(at, width), c0:c0 + w],
                               preferred_element_type=jnp.float32)
                if first:
                    total[:, c0:c0 + w] = part
                else:
                    total[:, c0:c0 + w] += part

        begun, relayed, squared, passed = False, False, [], []
        for op in ops:
            if op[0] == "send":
                along(*op[1:]).start()
            elif op[0] == "wait":
                if not begun:
                    begun = True
                    left_begin()
                along("y", 1, *op[1:]).wait_recv()
                if not relayed and op[2] > 40:
                    relayed = True
                    left_relay()
            elif op[0] == "pair":
                to_partner(*op[1:]).start()
            elif op[0] == "square":
                if not squared:
                    left_end()
                square_chunk(op[1])
                squared.append(op[1])
            elif len(squared) < len(chunks):
                relay_chunk(op[1])
                passed.append(op[1])
        for n in passed:
            far_chunk(n)
        rest = [n for n in squared if n not in passed]
        known = min(chunks[n][0] for n in rest)
        assert all(chunks[n][0] < known for n in passed)
        cube_part(0, 0, cols, first=True)
        for dx in (-1, 1, 2):
            cube_part(dx, 0, known)
        for n in rest:
            relay_chunk(n)
        cube_part(-1, known, cols - known)
        cube_part(1, known, cols - known)
        for n in rest:
            far_chunk(n)
        cube_part(2, known, cols - known)
        result = 3.0 * square[...] - 2.0 * (mask[...] * total[...])
        out_ref[...] = result
        current[...] = result.astype(jnp.bfloat16)

        sent = band.at[s, pl.ds(0, half - rows), :]
        pltpu.make_async_copy(sent, sent, band_send.at[s]).wait()
        shared = band.at[s, pl.ds(0, half), :]
        pltpu.make_async_copy(shared, shared, pair_send.at[s]).wait()
        for which in (0, 1):
            ref = left.at[s, which, :, pl.ds(0, 3 * cols)]
            pltpu.make_async_copy(ref, ref, left_send.at[s, which]).wait()
        return carry

    lax.fori_loop(0, STEPS, step, 0)


def solution(mesh):
    nx, ny, nz = mesh.shape["col"], mesh.shape["row"] // 2, mesh.shape["layer"]

    def shards(hamiltonian, tile_pattern, n_occ, mu, gamma):
        rows, cols = hamiltonian.shape
        order = nx * cols
        chunks = [(n * CHUNK, CHUNK, first) for n, first in CHUNKS]
        ops, count = gather_schedule(ny, nz, rows, chunks)
        vmem = pl.BlockSpec(memory_space=pltpu.VMEM)
        smem = pl.BlockSpec(memory_space=pltpu.SMEM)
        return pl.pallas_call(
            functools.partial(kernel, (nx, ny, nz, rows, cols), chunks, ops),
            out_shape=jax.ShapeDtypeStruct((rows, cols), jnp.float32),
            in_specs=[vmem, vmem, smem, smem, smem],
            out_specs=vmem,
            scratch_shapes=[
                pltpu.VMEM((STEPS, order, cols), jnp.bfloat16),
                pltpu.VMEM((STEPS, 2, rows, order), jnp.bfloat16),
                pltpu.VMEM((rows, cols), jnp.float32),
                pltpu.VMEM((rows, cols), jnp.float32),
                pltpu.VMEM((rows, cols), jnp.float32),
                pltpu.VMEM((rows, cols), jnp.bfloat16),
                pltpu.SemaphoreType.DMA((STEPS, count)),
                pltpu.SemaphoreType.DMA((STEPS,)),
                pltpu.SemaphoreType.DMA((STEPS, len(chunks))),
                pltpu.SemaphoreType.DMA((STEPS,)),
                pltpu.SemaphoreType.DMA((STEPS, 2, 4 * len(chunks))),
                pltpu.SemaphoreType.DMA((STEPS, 2)),
            ],
            compiler_params=pltpu.CompilerParams(
                collective_id=0, has_side_effects=True, vmem_limit_bytes=48 * 2**20),
            name="purify",
        )(hamiltonian, tile_pattern, n_occ, mu, gamma)

    placed = (P(("row", "layer"), "col"), P(), P(), P(), P())
    return jax.shard_map(
        shards, mesh=mesh, in_specs=placed, out_specs=P(("row", "layer"), "col"), check_vma=False
    )
```

```python
import functools
import heapq

import jax
import jax.numpy as jnp
from jax import lax
from jax.experimental import pallas as pl
from jax.experimental.pallas import tpu as pltpu
from jax.sharding import PartitionSpec as P

TILE = 128
LANES = 128
STEPS = 2
MESH = pl.DeviceIdType.MESH
CHUNK = 256
CHUNKS = ((0, 2, "y"), (2, 2, "y"), (4, 2, "z"), (6, 2, "z"), (8, 1, "z"), (9, 1, "z"))


def gather_schedule(ny, nz, rows, chunks, rate=46.65, lat=2.3, ahead=1.2, partner=1.5, late=5.1, hop=4.5,
                    issue=0.035, product=0.22):
    ring = {"y": ny, "z": nz}
    free, events, ops, waiting, tasks = {}, [], [], {}, []
    missing = {(n, dy): (nz - (dy == 0)) * c[1] for n, c in enumerate(chunks) for dy in range(ny)}
    parts = [0] * len(chunks)
    count = 0
    clock = 0.0

    def later(t, *event):
        heapq.heappush(events, (t, len(ops), len(events), *event))

    def offer(axis, sign, piece, hops):
        n, dy, dz, c0, w = piece
        half = ring[axis] // 2
        if hops == half:
            return
        if hops == half - 1:
            if w > LANES:
                cut = w // 2 // LANES * LANES
                piece = (n, dy, dz, c0, cut) if sign > 0 else (n, dy, dz, c0 + cut, w - cut)
            elif (sign > 0) != (c0 // LANES % 2 == 0):
                return
        second = axis != chunks[n][2]
        waiting.setdefault((axis, sign), []).append(((n + late * second, second, hops), piece, hops))

    def pump():
        nonlocal count, clock
        for (axis, sign), queue in waiting.items():
            while queue and free.get((axis, sign), 0.0) - ahead <= clock:
                queue.sort(key=lambda entry: entry[0])
                _, piece, hops = queue.pop(0)
                n, dy, dz, c0, w = piece
                clock += issue
                end = max(clock, free.get((axis, sign), 0.0)) + rows * w * 2 / rate / 1000
                free[axis, sign] = end
                ops.append(("send", axis, sign, piece, count))
                landed = (n, dy - sign, dz, c0, w) if axis == "y" else (n, dy, dz - sign, c0, w)
                later(end + lat, "land", axis, sign, landed, hops + 1, count)
                later(end - ahead, "free")
                count += 1

    for n, (c0, w, _) in enumerate(chunks):
        for axis in "yz":
            for sign in (1, -1):
                offer(axis, sign, (n, 0, 0, c0, w), 0)
    pump()
    while events or tasks:
        if tasks and (not events or events[0][0] > clock):
            n, dy = tasks.pop(0)
            ops.append(("part", n, dy, parts[n]))
            parts[n] += 1
            clock += product * max(chunks[n][1], CHUNK) / CHUNK
            if parts[n] == ny:
                ops.append(("finish", n))
                clock += 0.15
                later(clock + hop, "relay", n)
            continue
        t, _, _, kind, *rest = heapq.heappop(events)
        clock = max(clock, t)
        if kind == "land":
            axis, sign, piece, hops, receive = rest
            n, dy, dz, c0, w = piece
            ops.append(("wait", piece, receive))
            clock += issue
            offer(axis, sign, piece, hops)
            if axis == chunks[n][2]:
                for way in (1, -1):
                    offer("z" if axis == "y" else "y", way, piece, 0)
            missing[n, dy % ny] -= w
            if missing[n, dy % ny] == 0:
                ops.append(("pair", n, dy % ny))
                clock += issue
                later(clock + partner, "ready", n, dy % ny)
        elif kind == "ready":
            tasks.append(tuple(rest))
        elif kind == "relay":
            ops.append(("relay", rest[0]))
        pump()
    return ops, count


def spans(chunks):
    merged = []
    for c0, w, _ in sorted(chunks):
        if merged and sum(merged[-1]) == c0:
            merged[-1] = (merged[-1][0], merged[-1][1] + w)
        else:
            merged.append((c0, w))
    return merged


def kernel(sizes, chunks, ops, h_hbm, pattern_hbm, occ_ref, mu_ref, gamma_ref, out_ref,
           h_ref, pattern_ref, band, left, mask, square, total, current, band_recv, band_send, pair_recv, pair_send, left_recv, left_send, in_sem):
    nx, ny, nz, rows, cols = sizes
    order = nx * cols
    half = ny * nz * rows
    row, x, z = lax.axis_index("row"), lax.axis_index("col"), lax.axis_index("layer")
    y, core = row // 2, row % 2
    partner = {"row": 2 * y + 1 - core}
    to = {}
    for sign in (1, -1):
        to["x", sign] = {"col": (x + sign + nx) % nx}
        to["y", sign] = {"row": 2 * ((y + sign + ny) % ny) + core}
        to["z", sign] = {"layer": (z + sign + nz) % nz}
    row0 = pl.multiple_of((row * nz + z) * rows, 16)
    col0 = pl.multiple_of(x * cols, 128)

    h_copy = pltpu.make_async_copy(h_hbm, h_ref, in_sem.at[0])
    pattern_copy = pltpu.make_async_copy(pattern_hbm, pattern_ref, in_sem.at[1])
    pattern_copy.start()
    h_copy.start()
    barrier = pltpu.get_barrier_semaphore()
    friends = [partner, *to.values()]
    for friend in friends:
        pl.semaphore_signal(barrier, inc=1, device_id=friend, device_id_type=MESH)

    tiles = pattern_ref.shape[0]
    row_tile = (row0 + lax.broadcasted_iota(jnp.int32, (rows, tiles), 0)) // TILE
    row_hot = (row_tile == lax.broadcasted_iota(jnp.int32, (rows, tiles), 1)).astype(jnp.bfloat16)
    col_tile = (col0 + lax.broadcasted_iota(jnp.int32, (tiles, cols), 1)) // TILE
    col_hot = (col_tile == lax.broadcasted_iota(jnp.int32, (tiles, cols), 0)).astype(jnp.bfloat16)
    pattern_copy.wait()
    picked = jnp.dot(row_hot, pattern_ref[...].astype(jnp.float32).astype(jnp.bfloat16),
                     preferred_element_type=jnp.float32)
    mask[...] = jnp.dot(picked.astype(jnp.bfloat16), col_hot, preferred_element_type=jnp.float32)
    identity = (row0 + lax.broadcasted_iota(jnp.int32, (rows, cols), 0)
                == col0 + lax.broadcasted_iota(jnp.int32, (rows, cols), 1)).astype(jnp.float32)
    filling = occ_ref[0].astype(jnp.float32) / order
    h_copy.wait()
    start = mask[...] * (filling * identity + gamma_ref[0] * (mu_ref[0] * identity - h_ref[...].astype(jnp.float32)))
    current[...] = start.astype(jnp.bfloat16)

    pl.semaphore_wait(barrier, len(friends))

    def step(s, carry):
        def along(axis, sign, piece, receive):
            _, dy, dz, c0, w = piece
            origin = (2 * ((y + dy + ny) % ny) + core) * nz + (z + dz + nz) % nz
            ref = band.at[s, pl.ds(pl.multiple_of(origin * rows, 16), rows), pl.ds(c0, w)]
            return pltpu.make_async_remote_copy(
                src_ref=ref, dst_ref=ref, send_sem=band_send.at[s], recv_sem=band_recv.at[s, receive],
                device_id=to[axis, sign], device_id_type=MESH)

        def to_partner(n, dy):
            begin = pl.multiple_of((2 * ((y + dy) % ny) + core) * nz * rows, 16)
            ref = band.at[s, pl.ds(begin, nz * rows), pl.ds(*chunks[n][:2])]
            return pltpu.make_async_remote_copy(
                src_ref=ref, dst_ref=ref, send_sem=pair_send.at[s], recv_sem=pair_recv.at[s, ny * n + dy],
                device_id=partner, device_id_type=MESH)

        def along_x(which, sign, dx, c0, w, receive):
            at = pl.multiple_of(((x + dx + nx) % nx) * cols + c0, 128)
            ref = left.at[s, which, :, pl.ds(at, w)]
            return pltpu.make_async_remote_copy(
                src_ref=ref, dst_ref=ref, send_sem=left_send.at[s, which], recv_sem=left_recv.at[s, which, receive],
                device_id=to["x", sign], device_id_type=MESH)

        band[s, pl.ds(row0, rows), :] = current[...]
        left[s, 0, :, pl.ds(col0, cols)] = current[...]

        mid = cols // 2

        def left_begin():
            along_x(0, 1, 0, 0, cols, 0).start()
            along_x(0, -1, 0, 0, cols, 1).start()

        def left_relay():
            along_x(0, 1, -1, 0, cols, 0).wait_recv()
            along_x(0, 1, -1, 0, mid, 2).start()
            along_x(0, -1, 1, 0, cols, 1).wait_recv()
            along_x(0, -1, 1, mid, mid, 3).start()

        def left_end():
            along_x(0, 1, -2, 0, mid, 2).wait_recv()
            along_x(0, -1, -2, mid, mid, 3).wait_recv()

        def square_part(n, dy, turn):
            c0, w, _ = chunks[n]
            arrived = band.at[s, pl.ds(0, nz * rows), pl.ds(c0, w)]
            pltpu.make_async_copy(arrived, arrived, pair_recv.at[s, ny * n + dy]).wait()
            deep = 2 * nz * rows
            at = pl.multiple_of(((y + dy) % ny) * deep, 128)
            product = jnp.dot(left[s, 0, :, pl.ds(at, deep)], band[s, pl.ds(at, deep), c0:c0 + w],
                              preferred_element_type=jnp.float32)
            if turn == 0:
                square[:, c0:c0 + w] = product
            elif turn < ny - 1:
                square[:, c0:c0 + w] += product
            else:
                product = mask[:, c0:c0 + w] * (square[:, c0:c0 + w] + product)
                square[:, c0:c0 + w] = product
                left[s, 1, :, pl.ds(pl.multiple_of(col0 + c0, 128), w)] = product.astype(jnp.bfloat16)

        def square_send(n):
            c0, w, _ = chunks[n]
            along_x(1, 1, 0, c0, w, 4 * n).start()
            along_x(1, -1, 0, c0, w, 4 * n + 1).start()

        def far_parts(n):
            c0, w, _ = chunks[n]
            cut = (w // 2 + LANES * (1 - c0 // LANES % 2) // 2) // LANES * LANES
            return [part for part in ((1, c0, cut, 4 * n + 2), (-1, c0 + cut, w - cut, 4 * n + 3)) if part[2]]

        def relay_chunk(n):
            c0, w, _ = chunks[n]
            for sign, begin, width, receive in far_parts(n):
                along_x(1, sign, -sign, c0, w, receive - 2).wait_recv()
                along_x(1, sign, -sign, begin, width, receive).start()

        def near_chunk(n):
            c0, w, _ = chunks[n]
            for sign in {1, -1} - {part[0] for part in far_parts(n)}:
                along_x(1, sign, -sign, c0, w, 4 * n + (0 if sign > 0 else 1)).wait_recv()

        def far_chunk(n):
            for sign, begin, width, receive in far_parts(n):
                along_x(1, sign, -2, begin, width, receive).wait_recv()

        def cube_part(dx, ranges, first=False):
            for k0, width in ranges:
                at = pl.multiple_of(((x + dx + nx) % nx) * cols + k0, 128)
                for c0 in range(0, cols, CHUNK):
                    part = jnp.dot(left[s, 1, :, pl.ds(at, width)], band[s, pl.ds(at, width), c0:c0 + CHUNK],
                                   preferred_element_type=jnp.float32)
                    if first:
                        total[:, c0:c0 + CHUNK] = part
                    else:
                        total[:, c0:c0 + CHUNK] += part

        begun, relayed, started, done, passed = False, False, False, [], []
        for op in ops:
            if op[0] == "send":
                along(*op[1:]).start()
            elif op[0] == "wait":
                if not begun:
                    begun = True
                    left_begin()
                along("y", 1, *op[1:]).wait_recv()
                if not relayed and op[2] > 60:
                    relayed = True
                    left_relay()
            elif op[0] == "pair":
                to_partner(*op[1:]).start()
            elif op[0] == "part":
                if not started:
                    started = True
                    left_end()
                square_part(*op[1:])
            elif op[0] == "finish":
                square_send(op[1])
                done.append(op[1])
            elif len(done) < len(chunks):
                relay_chunk(op[1])
                passed.append(op[1])
        rest = [n for n in done if n not in passed]
        early, late = spans([chunks[n] for n in passed]), spans([chunks[n] for n in rest])
        cube_part(0, [(0, cols)], first=True)
        relay_chunk(rest[0])
        for n in passed:
            near_chunk(n)
            far_chunk(n)
        for dx in (-1, 1, 2):
            cube_part(dx, early)
        for n in rest[1:]:
            relay_chunk(n)
        for n in rest:
            near_chunk(n)
        cube_part(-1, late)
        cube_part(1, late)
        for n in rest:
            far_chunk(n)
        cube_part(2, late)
        result = 3.0 * square[...] - 2.0 * (mask[...] * total[...])
        out_ref[...] = result
        current[...] = result.astype(jnp.bfloat16)

        sent = band.at[s, pl.ds(0, half - rows), :]
        pltpu.make_async_copy(sent, sent, band_send.at[s]).wait()
        shared = band.at[s, pl.ds(0, half), :]
        pltpu.make_async_copy(shared, shared, pair_send.at[s]).wait()
        for which in (0, 1):
            ref = left.at[s, which, :, pl.ds(0, 3 * cols)]
            pltpu.make_async_copy(ref, ref, left_send.at[s, which]).wait()
        return carry

    lax.fori_loop(0, STEPS, step, 0)


def solution(mesh):
    nx, ny, nz = mesh.shape["col"], mesh.shape["row"] // 2, mesh.shape["layer"]

    def shards(hamiltonian, tile_pattern, n_occ, mu, gamma):
        rows, cols = hamiltonian.shape
        order = nx * cols
        chunks = [(n * LANES, w * LANES, first) for n, w, first in CHUNKS]
        ops, count = gather_schedule(ny, nz, rows, chunks)
        hbm = pl.BlockSpec(memory_space=pltpu.HBM)
        vmem = pl.BlockSpec(memory_space=pltpu.VMEM)
        smem = pl.BlockSpec(memory_space=pltpu.SMEM)
        return pl.pallas_call(
            functools.partial(kernel, (nx, ny, nz, rows, cols), chunks, ops),
            out_shape=jax.ShapeDtypeStruct((rows, cols), jnp.float32),
            in_specs=[hbm, hbm, smem, smem, smem],
            out_specs=vmem,
            scratch_shapes=[
                pltpu.VMEM((rows, cols), jnp.bfloat16),
                pltpu.VMEM(tile_pattern.shape, jnp.int32),
                pltpu.VMEM((STEPS, order, cols), jnp.bfloat16),
                pltpu.VMEM((STEPS, 2, rows, order), jnp.bfloat16),
                pltpu.VMEM((rows, cols), jnp.float32),
                pltpu.VMEM((rows, cols), jnp.float32),
                pltpu.VMEM((rows, cols), jnp.float32),
                pltpu.VMEM((rows, cols), jnp.bfloat16),
                pltpu.SemaphoreType.DMA((STEPS, count)),
                pltpu.SemaphoreType.DMA((STEPS,)),
                pltpu.SemaphoreType.DMA((STEPS, ny * len(chunks))),
                pltpu.SemaphoreType.DMA((STEPS,)),
                pltpu.SemaphoreType.DMA((STEPS, 2, 4 * len(chunks))),
                pltpu.SemaphoreType.DMA((STEPS, 2)),
                pltpu.SemaphoreType.DMA((2,)),
            ],
            compiler_params=pltpu.CompilerParams(
                collective_id=0, has_side_effects=True, vmem_limit_bytes=48 * 2**20),
            name="purify",
        )(hamiltonian, tile_pattern, n_occ, mu, gamma)

    placed = (P(("row", "layer"), "col"), P(), P(), P(), P())
    return jax.shard_map(
        shards, mesh=mesh, in_specs=placed, out_specs=P(("row", "layer"), "col"), check_vma=False
    )
```

```python
import functools
import heapq

import jax
import jax.numpy as jnp
from jax import lax
from jax.experimental import pallas as pl
from jax.experimental.pallas import tpu as pltpu
from jax.sharding import PartitionSpec as P

TILE = 128
LANES = 128
STEPS = 2
MESH = pl.DeviceIdType.MESH
CHUNK = 256
CHUNKS = ((0, 1, "y"), (1, 2, "y"), (3, 2, "z"), (5, 2, "z"), (7, 2, "z"), (9, 1, "y"))


def gather_schedule(ny, nz, rows, chunks, rate=46.65, lat=2.3, ahead=1.2, partner=1.5, late=5.1, hop=4.5,
                    issue=0.035, product=0.22):
    ring = {"y": ny, "z": nz}
    free, events, ops, waiting, tasks = {}, [], [], {}, []
    missing = {(n, dy): (nz - (dy == 0)) * c[1] for n, c in enumerate(chunks) for dy in range(ny)}
    parts = [0] * len(chunks)
    count = 0
    clock = 0.0

    def later(t, *event):
        heapq.heappush(events, (t, len(ops), len(events), *event))

    def offer(axis, sign, piece, hops):
        n, dy, dz, c0, w = piece
        half = ring[axis] // 2
        if hops == half:
            return
        if hops == half - 1:
            if w > LANES:
                cut = w // 2 // LANES * LANES
                piece = (n, dy, dz, c0, cut) if sign > 0 else (n, dy, dz, c0 + cut, w - cut)
            elif (sign > 0) != (c0 // LANES % 2 == 0):
                return
        second = axis != chunks[n][2]
        waiting.setdefault((axis, sign), []).append(((n + late * second, second, hops), piece, hops))

    def pump():
        nonlocal count, clock
        for (axis, sign), queue in waiting.items():
            while queue and free.get((axis, sign), 0.0) - ahead <= clock:
                queue.sort(key=lambda entry: entry[0])
                _, piece, hops = queue.pop(0)
                n, dy, dz, c0, w = piece
                clock += issue
                end = max(clock, free.get((axis, sign), 0.0)) + rows * w * 2 / rate / 1000
                free[axis, sign] = end
                ops.append(("send", axis, sign, piece, count))
                landed = (n, dy - sign, dz, c0, w) if axis == "y" else (n, dy, dz - sign, c0, w)
                later(end + lat, "land", axis, sign, landed, hops + 1, count)
                later(end - ahead, "free")
                count += 1

    for n, (c0, w, _) in enumerate(chunks):
        for axis in "yz":
            for sign in (1, -1):
                offer(axis, sign, (n, 0, 0, c0, w), 0)
    pump()
    while events or tasks:
        if tasks and (not events or events[0][0] > clock):
            n, dy = tasks.pop(0)
            ops.append(("part", n, dy, parts[n]))
            parts[n] += 1
            clock += product * max(chunks[n][1], CHUNK) / CHUNK
            if parts[n] == ny:
                ops.append(("finish", n))
                clock += 0.15
                later(clock + hop, "relay", n)
            continue
        t, _, _, kind, *rest = heapq.heappop(events)
        clock = max(clock, t)
        if kind == "land":
            axis, sign, piece, hops, receive = rest
            n, dy, dz, c0, w = piece
            ops.append(("wait", piece, receive))
            clock += issue
            offer(axis, sign, piece, hops)
            if axis == chunks[n][2]:
                for way in (1, -1):
                    offer("z" if axis == "y" else "y", way, piece, 0)
            missing[n, dy % ny] -= w
            if missing[n, dy % ny] == 0:
                ops.append(("pair", n, dy % ny))
                clock += issue
                later(clock + partner, "ready", n, dy % ny)
        elif kind == "ready":
            tasks.append(tuple(rest))
        elif kind == "relay":
            ops.append(("relay", rest[0]))
        pump()
    return ops, count


def spans(chunks):
    merged = []
    for c0, w, _ in sorted(chunks):
        if merged and sum(merged[-1]) == c0:
            merged[-1] = (merged[-1][0], merged[-1][1] + w)
        else:
            merged.append((c0, w))
    return merged


def kernel(sizes, chunks, ops, h_hbm, pattern_hbm, occ_hbm, mu_hbm, gamma_hbm, out_ref,
           h_ref, pattern_ref, occ_ref, mu_ref, gamma_ref, band, left, mask, square, total, current, band_recv, band_send, pair_recv, pair_send, left_recv, left_send, in_sem):
    nx, ny, nz, rows, cols = sizes
    order = nx * cols
    half = ny * nz * rows
    row, x, z = lax.axis_index("row"), lax.axis_index("col"), lax.axis_index("layer")
    y, core = row // 2, row % 2
    partner = {"row": 2 * y + 1 - core}
    to = {}
    for sign in (1, -1):
        to["x", sign] = {"col": (x + sign + nx) % nx}
        to["y", sign] = {"row": 2 * ((y + sign + ny) % ny) + core}
        to["z", sign] = {"layer": (z + sign + nz) % nz}
    row0 = pl.multiple_of((row * nz + z) * rows, 16)
    col0 = pl.multiple_of(x * cols, 128)

    h_copy = pltpu.make_async_copy(h_hbm, h_ref, in_sem.at[0])
    pattern_copy = pltpu.make_async_copy(pattern_hbm, pattern_ref, in_sem.at[1])
    scalar_copies = [pltpu.make_async_copy(hbm, ref, in_sem.at[2 + i]) for i, (hbm, ref) in enumerate(
        ((occ_hbm, occ_ref), (mu_hbm, mu_ref), (gamma_hbm, gamma_ref)))]
    for copy in (pattern_copy, h_copy, *scalar_copies):
        copy.start()
    barrier = pltpu.get_barrier_semaphore()
    friends = [partner, *to.values()]
    for friend in friends:
        pl.semaphore_signal(barrier, inc=1, device_id=friend, device_id_type=MESH)

    tiles = pattern_ref.shape[0]
    row_tile = (row0 + lax.broadcasted_iota(jnp.int32, (rows, tiles), 0)) // TILE
    row_hot = (row_tile == lax.broadcasted_iota(jnp.int32, (rows, tiles), 1)).astype(jnp.bfloat16)
    col_tile = (col0 + lax.broadcasted_iota(jnp.int32, (tiles, cols), 1)) // TILE
    col_hot = (col_tile == lax.broadcasted_iota(jnp.int32, (tiles, cols), 0)).astype(jnp.bfloat16)
    pattern_copy.wait()
    picked = jnp.dot(row_hot, pattern_ref[...].astype(jnp.float32).astype(jnp.bfloat16),
                     preferred_element_type=jnp.float32)
    mask[...] = jnp.dot(picked.astype(jnp.bfloat16), col_hot, preferred_element_type=jnp.float32)
    identity = (row0 + lax.broadcasted_iota(jnp.int32, (rows, cols), 0)
                == col0 + lax.broadcasted_iota(jnp.int32, (rows, cols), 1)).astype(jnp.float32)
    for copy in scalar_copies:
        copy.wait()
    filling = occ_ref[0].astype(jnp.float32) / order
    h_copy.wait()
    start = mask[...] * (filling * identity + gamma_ref[0] * (mu_ref[0] * identity - h_ref[...].astype(jnp.float32)))
    current[...] = start.astype(jnp.bfloat16)

    pl.semaphore_wait(barrier, len(friends))

    def step(s, carry):
        def along(axis, sign, piece, receive):
            _, dy, dz, c0, w = piece
            origin = (2 * ((y + dy + ny) % ny) + core) * nz + (z + dz + nz) % nz
            ref = band.at[s, pl.ds(pl.multiple_of(origin * rows, 16), rows), pl.ds(c0, w)]
            return pltpu.make_async_remote_copy(
                src_ref=ref, dst_ref=ref, send_sem=band_send.at[s], recv_sem=band_recv.at[s, receive],
                device_id=to[axis, sign], device_id_type=MESH)

        def to_partner(n, dy):
            begin = pl.multiple_of((2 * ((y + dy) % ny) + core) * nz * rows, 16)
            ref = band.at[s, pl.ds(begin, nz * rows), pl.ds(*chunks[n][:2])]
            return pltpu.make_async_remote_copy(
                src_ref=ref, dst_ref=ref, send_sem=pair_send.at[s], recv_sem=pair_recv.at[s, ny * n + dy],
                device_id=partner, device_id_type=MESH)

        def along_x(which, sign, dx, c0, w, receive):
            at = pl.multiple_of(((x + dx + nx) % nx) * cols + c0, 128)
            ref = left.at[s, which, :, pl.ds(at, w)]
            return pltpu.make_async_remote_copy(
                src_ref=ref, dst_ref=ref, send_sem=left_send.at[s, which], recv_sem=left_recv.at[s, which, receive],
                device_id=to["x", sign], device_id_type=MESH)

        band[s, pl.ds(row0, rows), :] = current[...]
        left[s, 0, :, pl.ds(col0, cols)] = current[...]

        mid = cols // 2

        def left_begin():
            along_x(0, 1, 0, 0, cols, 0).start()
            along_x(0, -1, 0, 0, cols, 1).start()

        def left_relay():
            along_x(0, 1, -1, 0, cols, 0).wait_recv()
            along_x(0, 1, -1, 0, mid, 2).start()
            along_x(0, -1, 1, 0, cols, 1).wait_recv()
            along_x(0, -1, 1, mid, mid, 3).start()

        def left_end():
            along_x(0, 1, -2, 0, mid, 2).wait_recv()
            along_x(0, -1, -2, mid, mid, 3).wait_recv()

        def square_part(n, dy, turn):
            c0, w, _ = chunks[n]
            arrived = band.at[s, pl.ds(0, nz * rows), pl.ds(c0, w)]
            pltpu.make_async_copy(arrived, arrived, pair_recv.at[s, ny * n + dy]).wait()
            deep = 2 * nz * rows
            at = pl.multiple_of(((y + dy) % ny) * deep, 128)
            product = jnp.dot(left[s, 0, :, pl.ds(at, deep)], band[s, pl.ds(at, deep), c0:c0 + w],
                              preferred_element_type=jnp.float32)
            if turn == 0:
                square[:, c0:c0 + w] = product
            elif turn < ny - 1:
                square[:, c0:c0 + w] += product
            else:
                product = mask[:, c0:c0 + w] * (square[:, c0:c0 + w] + product)
                square[:, c0:c0 + w] = product
                left[s, 1, :, pl.ds(pl.multiple_of(col0 + c0, 128), w)] = product.astype(jnp.bfloat16)

        def square_send(n):
            c0, w, _ = chunks[n]
            along_x(1, 1, 0, c0, w, 4 * n).start()
            along_x(1, -1, 0, c0, w, 4 * n + 1).start()

        def far_parts(n):
            c0, w, _ = chunks[n]
            cut = (w // 2 + LANES * (1 - c0 // LANES % 2) // 2) // LANES * LANES
            return [part for part in ((1, c0, cut, 4 * n + 2), (-1, c0 + cut, w - cut, 4 * n + 3)) if part[2]]

        def relay_chunk(n):
            c0, w, _ = chunks[n]
            for sign, begin, width, receive in far_parts(n):
                along_x(1, sign, -sign, c0, w, receive - 2).wait_recv()
                along_x(1, sign, -sign, begin, width, receive).start()

        def near_chunk(n):
            c0, w, _ = chunks[n]
            for sign in {1, -1} - {part[0] for part in far_parts(n)}:
                along_x(1, sign, -sign, c0, w, 4 * n + (0 if sign > 0 else 1)).wait_recv()

        def far_chunk(n):
            for sign, begin, width, receive in far_parts(n):
                along_x(1, sign, -2, begin, width, receive).wait_recv()

        def cube_part(dx, ranges, first=False):
            for k0, width in ranges:
                at = pl.multiple_of(((x + dx + nx) % nx) * cols + k0, 128)
                for c0 in range(0, cols, CHUNK):
                    part = jnp.dot(left[s, 1, :, pl.ds(at, width)], band[s, pl.ds(at, width), c0:c0 + CHUNK],
                                   preferred_element_type=jnp.float32)
                    if first:
                        total[:, c0:c0 + CHUNK] = part
                    else:
                        total[:, c0:c0 + CHUNK] += part

        begun, relayed, started, done, passed = False, False, False, [], []
        for op in ops:
            if op[0] == "send":
                along(*op[1:]).start()
            elif op[0] == "wait":
                if not begun:
                    begun = True
                    left_begin()
                along("y", 1, *op[1:]).wait_recv()
                if not relayed and op[2] > 60:
                    relayed = True
                    left_relay()
            elif op[0] == "pair":
                to_partner(*op[1:]).start()
            elif op[0] == "part":
                if not started:
                    started = True
                    left_end()
                square_part(*op[1:])
            elif op[0] == "finish":
                square_send(op[1])
                done.append(op[1])
            elif len(done) < len(chunks):
                relay_chunk(op[1])
                passed.append(op[1])
        rest = [n for n in done if n not in passed]
        early, late = spans([chunks[n] for n in passed]), spans([chunks[n] for n in rest])
        cube_part(0, [(0, cols)], first=True)
        relay_chunk(rest[0])
        for n in passed:
            near_chunk(n)
            far_chunk(n)
        for dx in (-1, 1, 2):
            cube_part(dx, early)
        for n in rest[1:]:
            relay_chunk(n)
        for n in rest:
            near_chunk(n)
        cube_part(-1, late)
        cube_part(1, late)
        for n in rest:
            far_chunk(n)
        cube_part(2, late)
        result = 3.0 * square[...] - 2.0 * (mask[...] * total[...])
        out_ref[...] = result
        current[...] = result.astype(jnp.bfloat16)

        sent = band.at[s, pl.ds(0, half - rows), :]
        pltpu.make_async_copy(sent, sent, band_send.at[s]).wait()
        shared = band.at[s, pl.ds(0, half), :]
        pltpu.make_async_copy(shared, shared, pair_send.at[s]).wait()
        for which in (0, 1):
            ref = left.at[s, which, :, pl.ds(0, 3 * cols)]
            pltpu.make_async_copy(ref, ref, left_send.at[s, which]).wait()
        return carry

    lax.fori_loop(0, STEPS, step, 0)


def solution(mesh):
    nx, ny, nz = mesh.shape["col"], mesh.shape["row"] // 2, mesh.shape["layer"]

    def shards(hamiltonian, tile_pattern, n_occ, mu, gamma):
        rows, cols = hamiltonian.shape
        order = nx * cols
        chunks = [(n * LANES, w * LANES, first) for n, w, first in CHUNKS]
        ops, count = gather_schedule(ny, nz, rows, chunks)
        hbm = pl.BlockSpec(memory_space=pltpu.HBM)
        vmem = pl.BlockSpec(memory_space=pltpu.VMEM)
        return pl.pallas_call(
            functools.partial(kernel, (nx, ny, nz, rows, cols), chunks, ops),
            out_shape=jax.ShapeDtypeStruct((rows, cols), jnp.float32),
            in_specs=[hbm] * 5,
            out_specs=vmem,
            scratch_shapes=[
                pltpu.VMEM((rows, cols), jnp.bfloat16),
                pltpu.VMEM(tile_pattern.shape, jnp.int32),
                pltpu.SMEM((1,), jnp.int32),
                pltpu.SMEM((1,), jnp.float32),
                pltpu.SMEM((1,), jnp.float32),
                pltpu.VMEM((STEPS, order, cols), jnp.bfloat16),
                pltpu.VMEM((STEPS, 2, rows, order), jnp.bfloat16),
                pltpu.VMEM((rows, cols), jnp.float32),
                pltpu.VMEM((rows, cols), jnp.float32),
                pltpu.VMEM((rows, cols), jnp.float32),
                pltpu.VMEM((rows, cols), jnp.bfloat16),
                pltpu.SemaphoreType.DMA((STEPS, count)),
                pltpu.SemaphoreType.DMA((STEPS,)),
                pltpu.SemaphoreType.DMA((STEPS, ny * len(chunks))),
                pltpu.SemaphoreType.DMA((STEPS,)),
                pltpu.SemaphoreType.DMA((STEPS, 2, 4 * len(chunks))),
                pltpu.SemaphoreType.DMA((STEPS, 2)),
                pltpu.SemaphoreType.DMA((5,)),
            ],
            compiler_params=pltpu.CompilerParams(
                collective_id=0, has_side_effects=True, vmem_limit_bytes=48 * 2**20),
            name="purify",
        )(*(pltpu.with_memory_space_constraint(v, pltpu.HBM) for v in (hamiltonian, tile_pattern)), n_occ, mu, gamma)

    placed = (P(("row", "layer"), "col"), P(), P(), P(), P())
    return jax.shard_map(
        shards, mesh=mesh, in_specs=placed, out_specs=P(("row", "layer"), "col"), check_vma=False
    )
```

```python
import functools
import heapq

import jax
import jax.numpy as jnp
from jax import lax
from jax.experimental import pallas as pl
from jax.experimental.pallas import tpu as pltpu
from jax.sharding import PartitionSpec as P

TILE = 128
LANES = 128
STEPS = 2
MESH = pl.DeviceIdType.MESH
CHUNK = 256
CHUNKS = ((0, 2, "y"), (2, 1, "y"), (3, 2, "z"), (5, 2, "z"), (7, 2, "z"), (9, 1, "y"))


def gather_schedule(ny, nz, rows, chunks, rate=46.65, lat=2.3, ahead=1.45, partner=1.5, late=5.1, hop=4.5,
                    issue=0.035, product=0.3):
    ring = {"y": ny, "z": nz}
    free, events, ops, waiting, tasks = {}, [], [], {}, []
    missing = {(n, dy): (nz - (dy == 0)) * c[1] for n, c in enumerate(chunks) for dy in range(ny)}
    parts = [0] * len(chunks)
    count = 0
    clock = 0.0

    def later(t, *event):
        heapq.heappush(events, (t, len(ops), len(events), *event))

    def offer(axis, sign, piece, hops):
        n, dy, dz, c0, w = piece
        half = ring[axis] // 2
        if hops == half:
            return
        if hops == half - 1:
            if w > LANES:
                cut = w // 2 // LANES * LANES
                piece = (n, dy, dz, c0, cut) if sign > 0 else (n, dy, dz, c0 + cut, w - cut)
            elif (sign > 0) != (c0 // LANES % 2 == 0):
                return
        second = axis != chunks[n][2]
        waiting.setdefault((axis, sign), []).append(((n + late * second, second, hops), piece, hops))

    def pump():
        nonlocal count, clock
        for (axis, sign), queue in waiting.items():
            while queue and free.get((axis, sign), 0.0) - ahead <= clock:
                queue.sort(key=lambda entry: entry[0])
                _, piece, hops = queue.pop(0)
                n, dy, dz, c0, w = piece
                clock += issue
                end = max(clock, free.get((axis, sign), 0.0)) + rows * w * 2 / rate / 1000
                free[axis, sign] = end
                ops.append(("send", axis, sign, piece, count))
                landed = (n, dy - sign, dz, c0, w) if axis == "y" else (n, dy, dz - sign, c0, w)
                later(end + lat, "land", axis, sign, landed, hops + 1, count)
                later(end - ahead, "free")
                count += 1

    for n, (c0, w, _) in enumerate(chunks):
        for axis in "yz":
            for sign in (1, -1):
                offer(axis, sign, (n, 0, 0, c0, w), 0)
    pump()
    while events or tasks:
        if tasks and (not events or events[0][0] > clock):
            n, dy = tasks.pop(0)
            ops.append(("part", n, dy, parts[n]))
            parts[n] += 1
            clock += product * max(chunks[n][1], CHUNK) / CHUNK
            if parts[n] == ny:
                ops.append(("finish", n))
                clock += 0.15
                later(clock + hop, "relay", n)
            continue
        t, _, _, kind, *rest = heapq.heappop(events)
        clock = max(clock, t)
        if kind == "land":
            axis, sign, piece, hops, receive = rest
            n, dy, dz, c0, w = piece
            ops.append(("wait", piece, receive))
            clock += issue
            offer(axis, sign, piece, hops)
            if axis == chunks[n][2]:
                for way in (1, -1):
                    offer("z" if axis == "y" else "y", way, piece, 0)
            missing[n, dy % ny] -= w
            if missing[n, dy % ny] == 0:
                ops.append(("pair", n, dy % ny))
                clock += issue
                later(clock + partner, "ready", n, dy % ny)
        elif kind == "ready":
            tasks.append(tuple(rest))
        elif kind == "relay":
            ops.append(("relay", rest[0]))
        pump()
    return ops, count


def spans(chunks):
    merged = []
    for c0, w, _ in sorted(chunks):
        if merged and sum(merged[-1]) == c0:
            merged[-1] = (merged[-1][0], merged[-1][1] + w)
        else:
            merged.append((c0, w))
    return merged


def kernel(sizes, chunks, ops, h_hbm, pattern_hbm, occ_hbm, mu_hbm, gamma_hbm, out_ref,
           h_ref, pattern_ref, occ_ref, mu_ref, gamma_ref, band, left, mask, square, total, current, band_recv, band_send, pair_recv, pair_send, left_recv, left_send, in_sem):
    nx, ny, nz, rows, cols = sizes
    order = nx * cols
    half = ny * nz * rows
    row, x, z = lax.axis_index("row"), lax.axis_index("col"), lax.axis_index("layer")
    y, core = row // 2, row % 2
    partner = {"row": 2 * y + 1 - core}
    to = {}
    for sign in (1, -1):
        to["x", sign] = {"col": (x + sign + nx) % nx}
        to["y", sign] = {"row": 2 * ((y + sign + ny) % ny) + core}
        to["z", sign] = {"layer": (z + sign + nz) % nz}
    row0 = pl.multiple_of((row * nz + z) * rows, 16)
    col0 = pl.multiple_of(x * cols, 128)

    h_copy = pltpu.make_async_copy(h_hbm, h_ref, in_sem.at[0])
    pattern_copy = pltpu.make_async_copy(pattern_hbm, pattern_ref, in_sem.at[1])
    scalar_copies = [pltpu.make_async_copy(hbm, ref, in_sem.at[2 + i]) for i, (hbm, ref) in enumerate(
        ((occ_hbm, occ_ref), (mu_hbm, mu_ref), (gamma_hbm, gamma_ref)))]
    for copy in (pattern_copy, h_copy, *scalar_copies):
        copy.start()
    barrier = pltpu.get_barrier_semaphore()
    friends = [partner, *to.values()]
    for friend in friends:
        pl.semaphore_signal(barrier, inc=1, device_id=friend, device_id_type=MESH)

    tiles = pattern_ref.shape[0]
    row_tile = (row0 + lax.broadcasted_iota(jnp.int32, (rows, tiles), 0)) // TILE
    row_hot = (row_tile == lax.broadcasted_iota(jnp.int32, (rows, tiles), 1)).astype(jnp.bfloat16)
    col_tile = (col0 + lax.broadcasted_iota(jnp.int32, (tiles, cols), 1)) // TILE
    col_hot = (col_tile == lax.broadcasted_iota(jnp.int32, (tiles, cols), 0)).astype(jnp.bfloat16)
    pattern_copy.wait()
    picked = jnp.dot(row_hot, pattern_ref[...].astype(jnp.float32).astype(jnp.bfloat16),
                     preferred_element_type=jnp.float32)
    mask[...] = jnp.dot(picked.astype(jnp.bfloat16), col_hot, preferred_element_type=jnp.float32)
    identity = (row0 + lax.broadcasted_iota(jnp.int32, (rows, cols), 0)
                == col0 + lax.broadcasted_iota(jnp.int32, (rows, cols), 1)).astype(jnp.float32)
    for copy in scalar_copies:
        copy.wait()
    filling = occ_ref[0].astype(jnp.float32) / order
    h_copy.wait()
    start = mask[...] * (filling * identity + gamma_ref[0] * (mu_ref[0] * identity - h_ref[...].astype(jnp.float32)))
    current[...] = start.astype(jnp.bfloat16)

    pl.semaphore_wait(barrier, len(friends))

    def step(s, carry):
        def along(axis, sign, piece, receive):
            _, dy, dz, c0, w = piece
            origin = (2 * ((y + dy + ny) % ny) + core) * nz + (z + dz + nz) % nz
            ref = band.at[s, pl.ds(pl.multiple_of(origin * rows, 16), rows), pl.ds(c0, w)]
            return pltpu.make_async_remote_copy(
                src_ref=ref, dst_ref=ref, send_sem=band_send.at[s], recv_sem=band_recv.at[s, receive],
                device_id=to[axis, sign], device_id_type=MESH)

        def to_partner(n, dy):
            begin = pl.multiple_of((2 * ((y + dy) % ny) + core) * nz * rows, 16)
            ref = band.at[s, pl.ds(begin, nz * rows), pl.ds(*chunks[n][:2])]
            return pltpu.make_async_remote_copy(
                src_ref=ref, dst_ref=ref, send_sem=pair_send.at[s], recv_sem=pair_recv.at[s, ny * n + dy],
                device_id=partner, device_id_type=MESH)

        def along_x(which, sign, dx, c0, w, receive):
            at = pl.multiple_of(((x + dx + nx) % nx) * cols + c0, 128)
            ref = left.at[s, which, :, pl.ds(at, w)]
            return pltpu.make_async_remote_copy(
                src_ref=ref, dst_ref=ref, send_sem=left_send.at[s, which], recv_sem=left_recv.at[s, which, receive],
                device_id=to["x", sign], device_id_type=MESH)

        band[s, pl.ds(row0, rows), :] = current[...]
        left[s, 0, :, pl.ds(col0, cols)] = current[...]

        mid = cols // 2

        def left_begin():
            along_x(0, 1, 0, 0, cols, 0).start()
            along_x(0, -1, 0, 0, cols, 1).start()

        def left_relay():
            along_x(0, 1, -1, 0, cols, 0).wait_recv()
            along_x(0, 1, -1, 0, mid, 2).start()
            along_x(0, -1, 1, 0, cols, 1).wait_recv()
            along_x(0, -1, 1, mid, mid, 3).start()

        def left_end():
            along_x(0, 1, -2, 0, mid, 2).wait_recv()
            along_x(0, -1, -2, mid, mid, 3).wait_recv()

        def square_part(n, dy, turn):
            c0, w, _ = chunks[n]
            arrived = band.at[s, pl.ds(0, nz * rows), pl.ds(c0, w)]
            pltpu.make_async_copy(arrived, arrived, pair_recv.at[s, ny * n + dy]).wait()
            deep = 2 * nz * rows
            at = pl.multiple_of(((y + dy) % ny) * deep, 128)
            product = jnp.dot(left[s, 0, :, pl.ds(at, deep)], band[s, pl.ds(at, deep), c0:c0 + w],
                              preferred_element_type=jnp.float32)
            if turn == 0:
                square[:, c0:c0 + w] = product
            elif turn < ny - 1:
                square[:, c0:c0 + w] += product
            else:
                product = mask[:, c0:c0 + w] * (square[:, c0:c0 + w] + product)
                square[:, c0:c0 + w] = product
                left[s, 1, :, pl.ds(pl.multiple_of(col0 + c0, 128), w)] = product.astype(jnp.bfloat16)

        def square_send(n):
            c0, w, _ = chunks[n]
            along_x(1, 1, 0, c0, w, 4 * n).start()
            along_x(1, -1, 0, c0, w, 4 * n + 1).start()

        def far_parts(n):
            c0, w, _ = chunks[n]
            cut = (w // 2 + LANES * (1 - c0 // LANES % 2) // 2) // LANES * LANES
            return [part for part in ((1, c0, cut, 4 * n + 2), (-1, c0 + cut, w - cut, 4 * n + 3)) if part[2]]

        def relay_chunk(n):
            c0, w, _ = chunks[n]
            for sign, begin, width, receive in far_parts(n):
                along_x(1, sign, -sign, c0, w, receive - 2).wait_recv()
                along_x(1, sign, -sign, begin, width, receive).start()

        def near_chunk(n):
            c0, w, _ = chunks[n]
            for sign in {1, -1} - {part[0] for part in far_parts(n)}:
                along_x(1, sign, -sign, c0, w, 4 * n + (0 if sign > 0 else 1)).wait_recv()

        def far_chunk(n):
            for sign, begin, width, receive in far_parts(n):
                along_x(1, sign, -2, begin, width, receive).wait_recv()

        def cube_part(dx, ranges, first=False):
            for k0, width in ranges:
                at = pl.multiple_of(((x + dx + nx) % nx) * cols + k0, 128)
                for c0 in range(0, cols, CHUNK):
                    part = jnp.dot(left[s, 1, :, pl.ds(at, width)], band[s, pl.ds(at, width), c0:c0 + CHUNK],
                                   preferred_element_type=jnp.float32)
                    if first:
                        total[:, c0:c0 + CHUNK] = part
                    else:
                        total[:, c0:c0 + CHUNK] += part

        begun, relayed, started, done, passed = False, False, False, [], []
        for op in ops:
            if op[0] == "send":
                along(*op[1:]).start()
            elif op[0] == "wait":
                if not begun:
                    begun = True
                    left_begin()
                along("y", 1, *op[1:]).wait_recv()
                if not relayed and op[2] > 60:
                    relayed = True
                    left_relay()
            elif op[0] == "pair":
                to_partner(*op[1:]).start()
            elif op[0] == "part":
                if not started:
                    started = True
                    left_end()
                square_part(*op[1:])
            elif op[0] == "finish":
                square_send(op[1])
                done.append(op[1])
            elif len(done) < len(chunks):
                relay_chunk(op[1])
                passed.append(op[1])
        rest = [n for n in done if n not in passed]
        early, late = spans([chunks[n] for n in passed]), spans([chunks[n] for n in rest])
        cube_part(0, [(0, cols)], first=True)
        relay_chunk(rest[0])
        for n in passed:
            near_chunk(n)
            far_chunk(n)
        for dx in (-1, 1, 2):
            cube_part(dx, early)
        for n in rest[1:]:
            relay_chunk(n)
        for n in rest:
            near_chunk(n)
        cube_part(-1, late)
        cube_part(1, late)
        for n in rest:
            far_chunk(n)
        cube_part(2, late)
        result = 3.0 * square[...] - 2.0 * (mask[...] * total[...])
        out_ref[...] = result
        current[...] = result.astype(jnp.bfloat16)

        sent = band.at[s, pl.ds(0, half - rows), :]
        pltpu.make_async_copy(sent, sent, band_send.at[s]).wait()
        shared = band.at[s, pl.ds(0, half), :]
        pltpu.make_async_copy(shared, shared, pair_send.at[s]).wait()
        for which in (0, 1):
            ref = left.at[s, which, :, pl.ds(0, 3 * cols)]
            pltpu.make_async_copy(ref, ref, left_send.at[s, which]).wait()
        return carry

    lax.fori_loop(0, STEPS, step, 0)


def solution(mesh):
    nx, ny, nz = mesh.shape["col"], mesh.shape["row"] // 2, mesh.shape["layer"]

    def shards(hamiltonian, tile_pattern, n_occ, mu, gamma):
        rows, cols = hamiltonian.shape
        order = nx * cols
        chunks = [(n * LANES, w * LANES, first) for n, w, first in CHUNKS]
        ops, count = gather_schedule(ny, nz, rows, chunks)
        hbm = pl.BlockSpec(memory_space=pltpu.HBM)
        vmem = pl.BlockSpec(memory_space=pltpu.VMEM)
        return pl.pallas_call(
            functools.partial(kernel, (nx, ny, nz, rows, cols), chunks, ops),
            out_shape=jax.ShapeDtypeStruct((rows, cols), jnp.float32),
            in_specs=[hbm] * 5,
            out_specs=vmem,
            scratch_shapes=[
                pltpu.VMEM((rows, cols), jnp.bfloat16),
                pltpu.VMEM(tile_pattern.shape, jnp.int32),
                pltpu.SMEM((1,), jnp.int32),
                pltpu.SMEM((1,), jnp.float32),
                pltpu.SMEM((1,), jnp.float32),
                pltpu.VMEM((STEPS, order, cols), jnp.bfloat16),
                pltpu.VMEM((STEPS, 2, rows, order), jnp.bfloat16),
                pltpu.VMEM((rows, cols), jnp.float32),
                pltpu.VMEM((rows, cols), jnp.float32),
                pltpu.VMEM((rows, cols), jnp.float32),
                pltpu.VMEM((rows, cols), jnp.bfloat16),
                pltpu.SemaphoreType.DMA((STEPS, count)),
                pltpu.SemaphoreType.DMA((STEPS,)),
                pltpu.SemaphoreType.DMA((STEPS, ny * len(chunks))),
                pltpu.SemaphoreType.DMA((STEPS,)),
                pltpu.SemaphoreType.DMA((STEPS, 2, 4 * len(chunks))),
                pltpu.SemaphoreType.DMA((STEPS, 2)),
                pltpu.SemaphoreType.DMA((5,)),
            ],
            compiler_params=pltpu.CompilerParams(
                collective_id=0, has_side_effects=True, vmem_limit_bytes=48 * 2**20),
            name="purify",
        )(*(pltpu.with_memory_space_constraint(v, pltpu.HBM) for v in (hamiltonian, tile_pattern)), n_occ, mu, gamma)

    placed = (P(("row", "layer"), "col"), P(), P(), P(), P())
    return jax.shard_map(
        shards, mesh=mesh, in_specs=placed, out_specs=P(("row", "layer"), "col"), check_vma=False
    )
```
